32 devices in a mesh: band: 8 (over z, y), grid: 4 (over x, core).
Axes of the slice: x: 2, y: 2, z: 4, core: 2. Of those that a mesh axis runs over, the one named last changes fastest.
Arguments:
- orbitals: float32 [32, 110592], P('band', 'grid'), may hold values from -6 to 6
Outputs:
- exchange_vectors: float32 [32, 110592], P('band', 'grid')
- margin: float32 [32, 32], P('grid', 'band')
The draws below stay inside these ranges and needn't reach their ends.
All inputs are finite; a program needn't handle non-finite values.
Results may differ from the reference program's by a relative error of at most 0.00012.
Values sent between devices are 32-bit elements; how exact they have to be, the bound alone decides.
A program may use at most 128 MiB of HBM per device.

```python
import jax
import jax.numpy as jnp
from jax import lax

NG = 48
BAND_DEV = 4
NBANDS = 32
NCELL = 110592
N_BAND = 8


def steps_of(rng, dims, split, least, top_value):
    gain, own = 1.0, jax.random.fold_in(rng, 6)
    for position, shards_of in split:
        heights = jnp.exp(jax.random.uniform(jax.random.fold_in(own, position), (shards_of,), jnp.float32, least / len(split), top_value / len(split)))
        gain = gain * jnp.repeat(heights, dims[position] // shards_of).reshape([-1 if axis == position else 1 for axis in range(len(dims))])
    return gain


def normal_values(stream_key, shape, deviation, reach, split=(), kind=jnp.bfloat16):
    result = jax.random.normal(stream_key, shape, jnp.float32) * deviation
    if len(split) > 0:
        result = steps_of(stream_key, shape, split, -0.22, 0.18) * result
    return jnp.clip(result, min=-reach, max=reach).astype(kind)


def setup_inputs(seed: int = 0) -> dict:
    streams_of = jax.random.split(jax.random.key(seed), 2)
    orbitals = normal_values(streams_of[0], (NBANDS, NCELL), 1.0, 6.0, ((0, 8), (1, 4)), jnp.float32)
    return dict(orbitals=orbitals)


def folded_freq(count):
    indices = jnp.arange(count)
    return ((indices + count // 2) % count - count // 2).astype(jnp.float32)


def kernel_table():
    freqs = folded_freq(NG)
    squares = freqs[:, None, None] ** 2 + freqs[None, :, None] ** 2 + freqs[None, None, :] ** 2
    safe_sq = jnp.where(squares > 0, squares, jnp.float32(1.0))
    return jnp.where(squares > 0, 40.0 * (1.0 - jnp.exp(-squares / 16.0)) / safe_sq, jnp.float32(0.0))


def reference(orbitals):
    kernel = kernel_table()
    blocks = orbitals.reshape(N_BAND, BAND_DEV, NCELL)
    window = jnp.concatenate([blocks, jnp.roll(blocks, 1, axis=0), jnp.roll(blocks, -1, axis=0)], axis=1)

    def per_band(single, partners):
        density = (single[None, :] * partners).reshape(-1, NG, NG, NG)
        spectrum = jnp.fft.fftn(density, axes=(1, 2, 3))
        potential = jnp.real(jnp.fft.ifftn(spectrum * kernel, axes=(1, 2, 3))).reshape(-1, NCELL)
        return -jnp.sum(partners * potential, axis=0)

    def per_block(args):
        own_block, partners = args
        return lax.map(lambda single: per_band(single, partners), own_block)

    vectors = lax.map(per_block, (blocks, window)).reshape(NBANDS, NCELL).astype(jnp.float32)
    margin = jnp.dot(orbitals, vectors.T, precision=lax.Precision.HIGHEST, preferred_element_type=jnp.float32) / NCELL
    return vectors, margin
```

```python
import functools

import jax
import jax.numpy as jnp
import numpy as np
from jax import lax
from jax.experimental import pallas as pl
from jax.experimental.pallas import tpu as pltpu
from jax.sharding import PartitionSpec as P


def kernel_values(ng):
    freqs = ((np.arange(ng) + ng // 2) % ng - ng // 2).astype(np.float32)
    sq = freqs[: ng // 2 + 1, None, None] ** 2 + freqs[None, :, None] ** 2 + freqs[None, None, :] ** 2
    safe = np.where(sq > 0, sq, np.float32(1.0))
    return np.where(sq > 0, 40.0 * (1.0 - np.exp(-sq / 16.0)) / safe, 0.0)


def hartley(ng):
    k = np.arange(ng)
    ang = (k[:, None] * k[None, :] % ng) * (2.0 * np.pi / ng)
    return np.cos(ang) + np.sin(ang)


def split_const(table):
    table = np.asarray(table, np.float32)
    hi = table.astype(jnp.bfloat16)
    lo = (table - hi.astype(np.float32)).astype(jnp.bfloat16)
    return hi, lo


def rfft(xs):
    n = len(xs)
    if n == 3:
        s = xs[1] + xs[2]
        d = xs[1] - xs[2]
        return [(xs[0] + s, None), (xs[0] - 0.5 * s, d * (-np.sqrt(3.0) / 2))]
    even, odd = rfft(xs[0::2]), rfft(xs[1::2])
    half = n // 2
    out = [None] * (half + 1)
    for k in range(half // 2 + 1):
        er, ei = even[k]
        orr, oi = odd[k]
        if k == 0:
            out[0] = (er + orr, None)
            out[half] = (er - orr, None)
            continue
        c, s = np.cos(2 * np.pi * k / n), -np.sin(2 * np.pi * k / n)
        if 2 * k == half:
            out[k] = (er, -orr)
            continue
        tr, ti = cmul(orr, oi, c, s)
        out[k] = (er + tr, addo(ei, ti))
        out[half - k] = (er - tr, subo(ti, ei))
    return out


def addo(a, b):
    return b if a is None else a + b


def subo(a, b):
    return a if b is None else a - b


def cmul(r, i, c, s):
    if i is None:
        return r * c, r * s
    if abs(abs(c) - abs(s)) < 1e-9:
        if s < 0 < c:
            return (r + i) * c, (i - r) * c
        return (r - i) * c, (r + i) * c
    return r * c - i * s, r * s + i * c


def irfft(spec, n):
    if n == 3:
        dc, (r, i) = spec[0][0], spec[1]
        base = dc - r
        t = i * np.sqrt(3.0)
        return [dc + 2.0 * r, base - t, base + t]
    half = n // 2
    even, odd = [None] * (half // 2 + 1), [None] * (half // 2 + 1)
    for k in range(half // 2 + 1):
        yr, yi = spec[k]
        if k == 0:
            hr = spec[half][0]
            even[0] = (yr + hr, None)
            odd[0] = (yr - hr, None)
            continue
        if 2 * k == half:
            even[k] = (yr + yr, None)
            odd[k] = (-(yi + yi), None)
            continue
        zr, zi = spec[half - k]
        er, ei = yr + zr, yi - zi
        dr, di = yr - zr, yi + zi
        c, s = np.cos(2 * np.pi * k / n), np.sin(2 * np.pi * k / n)
        even[k] = (er, ei)
        odd[k] = cmul(dr, di, c, s)
    ev, od = irfft(even, half), irfft(odd, half)
    out = [None] * n
    out[0::2], out[1::2] = ev, od
    return out


def split(v):
    hi = v.astype(jnp.bfloat16)
    lo = (v - hi.astype(jnp.float32)).astype(jnp.bfloat16)
    return hi, lo


def mm(a, b):
    return jnp.dot(a, b, preferred_element_type=jnp.float32)


def solve_kernel(ng, rows, a_ref, b_ref, k_ref, zh_ref, zl_ref, ty_ref, s_ref, o_ref, work):
    width = b_ref.shape[-1]
    owed_w = (o_ref.shape[-1] // (ng * 5)) * ng * 4
    out_w = o_ref.shape[-1]

    def ztrans(v):
        hi, lo = split(v)
        return mm(hi, zh_ref[...]) + mm(lo, zh_ref[...]) + mm(hi, zl_ref[...])

    def ytrans(v):
        hi, lo = split(v)
        return mm(ty_ref[...], jnp.concatenate([hi, lo, hi], axis=0))

    def forward(c, _):
        base = c * rows
        p = (a_ref[pl.ds(base, rows)] * b_ref[pl.ds(base, rows)]).reshape(rows * ng, width)
        q = ztrans(p).reshape(rows, ng, width)
        for r in range(rows):
            work[base + r] = ytrans(q[r])
        return 0

    lax.fori_loop(0, ng // rows, forward, 0)

    def xconv(t, _):
        y0 = pl.multiple_of(t * 8, 8)
        for l in range(width // 128):
            sl = (pl.ds(y0, 8), pl.ds(l * 128, 128))
            spec = rfft([work[x, sl[0], sl[1]] for x in range(ng)])
            out = []
            for k, (re, im) in enumerate(spec):
                kv = k_ref[k, sl[0], sl[1]]
                out.append((re * kv, None if im is None else im * kv))
            res = irfft(out, ng)
            for x in range(ng):
                work[x, sl[0], sl[1]] = res[x]
        return 0

    lax.fori_loop(0, ng // 8, xconv, 0)

    def inverse(c, _):
        base = c * rows
        q = jnp.concatenate([ytrans(work[base + r]) for r in range(rows)], axis=0)
        pot = ztrans(q)
        b = b_ref[pl.ds(base, rows)].reshape(rows * ng, width)
        a = a_ref[pl.ds(base, rows)].reshape(rows * ng, width)
        hi, lo = split(b * pot)
        vec = mm(hi, s_ref[...]) + mm(lo, s_ref[...])
        owed = a[:, :out_w] * pot[:, :out_w]
        lane = lax.broadcasted_iota(jnp.int32, owed.shape, 1)
        res = jnp.where(lane < owed_w, owed, vec)
        o_ref[pl.ds(base, rows)] = (-res).reshape(rows, ng, out_w)
        return 0

    lax.fori_loop(0, ng // rows, inverse, 0)


def solve(a, b, bands):
    ng, width = a.shape[0], a.shape[-1]
    count = width // ng
    ht = hartley(ng)
    th, tl = split_const(ht)
    zh, zl = split_const(np.kron(np.eye(count), ht))
    ty = np.concatenate([th, th, tl], axis=1)
    out_w = (bands + 1) * ng
    sel = np.zeros((width, out_w), np.float32)
    for p in range(count):
        sel[p * ng + np.arange(ng), bands * ng + np.arange(ng)] = 1.0
    kv = kernel_values(ng).astype(np.float32)
    kv = np.tile(kv / np.float32(ng**3), (1, 1, count))
    rows = 6
    return pl.pallas_call(
        functools.partial(solve_kernel, ng, rows),
        out_shape=jax.ShapeDtypeStruct((ng, ng, out_w), jnp.float32),
        in_specs=[pl.BlockSpec(memory_space=pltpu.VMEM)] * 7,
        out_specs=pl.BlockSpec(memory_space=pltpu.VMEM),
        scratch_shapes=[pltpu.VMEM((ng, ng, width), jnp.float32)],
        compiler_params=pltpu.CompilerParams(vmem_limit_bytes=56 * 1024 * 1024),
        cost_estimate=pl.CostEstimate(flops=10**10, bytes_accessed=10**7, transcendentals=0),
        name="solve",
    )(a, b, jnp.asarray(kv), jnp.asarray(zh), jnp.asarray(zl), jnp.asarray(ty), jnp.asarray(sel, jnp.bfloat16))


def from_behind(value, axis, steps):
    count = lax.axis_size(axis)
    return lax.ppermute(value, axis, [(s, (s + steps) % count) for s in range(count)])


def on_device(orbitals):
    groups = lax.axis_size("grid")
    bands, local = orbitals.shape
    ncell = local * groups
    ng = round(ncell ** (1 / 3))
    xs = local // (ng * ng)
    own = orbitals.reshape(bands, xs, ng, ng).transpose(1, 2, 0, 3).reshape(xs, ng, bands * ng)
    lower = from_behind(own, "band", 1)
    both = lax.all_gather(jnp.concatenate([lower, own], axis=2), "grid", axis=0, tiled=True)
    me = lax.axis_index("grid")
    mine = lax.dynamic_slice_in_dim(both, (bands + me) * ng, ng, axis=2)
    out = solve(jnp.tile(mine, (1, 1, 2 * bands)), both, bands)
    recv = lax.all_to_all(out.reshape(groups, xs, ng, -1), "grid", split_axis=0, concat_axis=0, tiled=True)
    owed = from_behind(recv[..., : bands * ng].sum(axis=0), "band", -1)
    vec = recv[..., bands * ng :] + owed.reshape(xs, ng, bands, ng).transpose(2, 0, 1, 3)
    vectors = vec.reshape(bands, local)
    terms = (
        lax.dot_general(
            lax.all_gather(orbitals, "band", axis=0, tiled=True),
            vectors,
            (((1,), (1,)), ((), ())),
            precision=lax.Precision.HIGHEST,
            preferred_element_type=jnp.float32,
        )
        / ncell
    )
    margin = lax.psum_scatter(terms, "grid", scatter_dimension=0, tiled=True)
    return (vectors, margin)


def solution(mesh):
    return jax.shard_map(
        on_device,
        mesh=mesh,
        in_specs=(P("band", "grid"),),
        out_specs=(P("band", "grid"), P("grid", "band")),
        check_vma=False,
    )
```

```python
import functools

import jax
import jax.numpy as jnp
import numpy as np
from jax import lax
from jax.experimental import pallas as pl
from jax.experimental.pallas import tpu as pltpu
from jax.sharding import PartitionSpec as P


def kernel_values(ng):
    freqs = ((np.arange(ng) + ng // 2) % ng - ng // 2).astype(np.float32)
    sq = freqs[: ng // 2 + 1, None, None] ** 2 + freqs[None, :, None] ** 2 + freqs[None, None, :] ** 2
    safe = np.where(sq > 0, sq, np.float32(1.0))
    return np.where(sq > 0, 40.0 * (1.0 - np.exp(-sq / 16.0)) / safe, 0.0)


def hartley(ng):
    k = np.arange(ng)
    ang = (k[:, None] * k[None, :] % ng) * (2.0 * np.pi / ng)
    return np.cos(ang) + np.sin(ang)


def split_const(table):
    table = np.asarray(table, np.float32)
    hi = table.astype(jnp.bfloat16)
    lo = (table - hi.astype(np.float32)).astype(jnp.bfloat16)
    return hi, lo


def rfft(xs):
    n = len(xs)
    if n == 3:
        s = xs[1] + xs[2]
        d = xs[1] - xs[2]
        return [(xs[0] + s, None), (xs[0] - 0.5 * s, d * (-np.sqrt(3.0) / 2))]
    even, odd = rfft(xs[0::2]), rfft(xs[1::2])
    half = n // 2
    out = [None] * (half + 1)
    for k in range(half // 2 + 1):
        er, ei = even[k]
        orr, oi = odd[k]
        if k == 0:
            out[0] = (er + orr, None)
            out[half] = (er - orr, None)
            continue
        c, s = np.cos(2 * np.pi * k / n), -np.sin(2 * np.pi * k / n)
        if 2 * k == half:
            out[k] = (er, -orr)
            continue
        tr, ti = cmul(orr, oi, c, s)
        out[k] = (er + tr, addo(ei, ti))
        out[half - k] = (er - tr, subo(ti, ei))
    return out


def addo(a, b):
    return b if a is None else a + b


def subo(a, b):
    return a if b is None else a - b


def cmul(r, i, c, s):
    if i is None:
        return r * c, r * s
    if abs(abs(c) - abs(s)) < 1e-9:
        if s < 0 < c:
            return (r + i) * c, (i - r) * c
        return (r - i) * c, (r + i) * c
    return r * c - i * s, r * s + i * c


def irfft(spec, n):
    if n == 3:
        dc, (r, i) = spec[0][0], spec[1]
        base = dc - r
        t = i * np.sqrt(3.0)
        return [dc + 2.0 * r, base - t, base + t]
    half = n // 2
    even, odd = [None] * (half // 2 + 1), [None] * (half // 2 + 1)
    for k in range(half // 2 + 1):
        yr, yi = spec[k]
        if k == 0:
            hr = spec[half][0]
            even[0] = (yr + hr, None)
            odd[0] = (yr - hr, None)
            continue
        if 2 * k == half:
            even[k] = (yr + yr, None)
            odd[k] = (-(yi + yi), None)
            continue
        zr, zi = spec[half - k]
        er, ei = yr + zr, yi - zi
        dr, di = yr - zr, yi + zi
        c, s = np.cos(2 * np.pi * k / n), np.sin(2 * np.pi * k / n)
        even[k] = (er, ei)
        odd[k] = cmul(dr, di, c, s)
    ev, od = irfft(even, half), irfft(odd, half)
    out = [None] * n
    out[0::2], out[1::2] = ev, od
    return out


def split(v):
    hi = v.astype(jnp.bfloat16)
    lo = (v - hi.astype(jnp.float32)).astype(jnp.bfloat16)
    return hi, lo


def mm(a, b):
    return jnp.dot(a, b, preferred_element_type=jnp.float32)


def solve_kernel(ng, own_ref, k1_ref, k2_ref, zh_ref, zl_ref, ty_ref, sel_ref, s_ref, o_ref,
                 buf, amp, acc, work, vec, recv, rsem, ssem, nsem, osem, orsem, lsem):
    planes, _, width = own_ref.shape
    me = lax.axis_index("grid")
    band, nband = lax.axis_index("band"), lax.axis_size("band")
    chip, core = me // 2, me % 2
    sib = chip * 2 + (1 - core)
    cross = (1 - chip) * 2 + core
    far = (1 - chip) * 2 + (1 - core)
    above, below = (band + 1) % nband, (band + nband - 1) % nband
    mesh_id = pl.DeviceIdType.MESH

    def remote(src, dst, send, recv_sem, device):
        return pltpu.make_async_remote_copy(
            src_ref=src, dst_ref=dst, send_sem=send, recv_sem=recv_sem,
            device_id=device, device_id_type=mesh_id,
        )

    def share(blk, lane, slot, src, target):
        return remote(src, buf.at[blk, slot], ssem.at[blk, lane], rsem.at[blk, slot], (band, target))

    barrier = pltpu.get_barrier_semaphore()
    for device in ((band, sib), (band, cross), (band, far), (above, me), (below, me)):
        pl.semaphore_signal(barrier, inc=1, device_id=device, device_id_type=mesh_id)
    pl.semaphore_wait(barrier, 5)

    share(0, 1, me, own_ref, cross).start()
    share(0, 0, me, own_ref, sib).start()
    remote(own_ref, buf.at[1, me], nsem.at[0], rsem.at[1, me], (above, me)).start()
    remote(own_ref, buf.at[2, me], nsem.at[1], rsem.at[2, me], (below, me)).start()
    local = pltpu.make_async_copy(own_ref, buf.at[0, me], lsem)
    local.start()

    def arrived(blk, slot):
        share(blk, 0, slot, own_ref, sib).wait_recv()

    def relay(blk):
        arrived(blk, cross)
        share(blk, 2, cross, buf.at[blk, cross], sib).start()

    def spread(blk):
        arrived(blk, me)
        share(blk, 1, me, buf.at[blk, me], cross).start()
        share(blk, 0, me, buf.at[blk, me], sib).start()

    def ztrans(v):
        hi, lo = split(v)
        return mm(hi, zh_ref[...]) + mm(lo, zh_ref[...]) + mm(hi, zl_ref[...])

    def ytrans(v):
        hi, lo = split(v)
        return mm(ty_ref[...], jnp.concatenate([hi, lo, hi], axis=0))

    def slot_of(s):
        return ((chip + s // 2) % 2) * 2 + (core + s % 2) % 2

    def amplitude(slot):
        hi, lo = split(buf[0, slot].reshape(planes * ng, width))
        amp[slot] = (mm(hi, sel_ref[me]) + mm(lo, sel_ref[me])).reshape(planes, ng, width)

    def forward(blk, s):
        slot = slot_of(s)

        @pl.when(s == 1)
        def _():
            arrived(blk, sib)

        @pl.when(jnp.logical_and(blk == 0, s == 2))
        def _():
            relay(0)
            spread(1)

        @pl.when(s == 3)
        def _():
            arrived(blk, far)

        @pl.when(blk == 0)
        def _():
            amplitude(slot)

        p = (amp[slot] * buf[blk, slot]).reshape(planes * ng, width)
        q = ztrans(p).reshape(planes, ng, width)
        for r in range(planes):
            work[slot, r] = ytrans(q[r])

    def conv(vals, kern):
        spec = rfft(vals)
        out = []
        for k, (re, im) in enumerate(spec):
            kv = kern(k)
            out.append((re * kv, None if im is None else im * kv))
        return irfft(out, ng)

    def xconv(t):
        order = [(g, h, r) for g in range(4) for h in range(2) for r in range(planes)]
        for i in range(2):
            rows = pl.ds(pl.multiple_of(t * 16 + 8 * i, 8), 8)
            res = conv([work[g, r, rows, h * 128:h * 128 + 128] for g, h, r in order],
                       lambda k: k1_ref[k, rows, :])
            for (g, h, r), v in zip(order, res):
                work[g, r, rows, h * 128:h * 128 + 128] = v
        ra = pl.ds(pl.multiple_of(t * 16, 8), 8)
        rb = pl.ds(pl.multiple_of(t * 16 + 8, 8), 8)
        left = lax.broadcasted_iota(jnp.int32, (8, 128), 1) < 64

        def half(g, h, r):
            u, w = work[g, r, ra, 256:384], work[g, r, rb, 256:384]
            if h == 0:
                return jnp.where(left, u, pltpu.roll(w, 64, 1))
            return jnp.where(left, pltpu.roll(u, 64, 1), w)

        rk = pl.ds(pl.multiple_of(t * 8, 8), 8)
        res = dict(zip(order, conv([half(*o) for o in order], lambda k: k2_ref[k, rk, :])))
        for g in range(4):
            for r in range(planes):
                a, b = res[(g, 0, r)], res[(g, 1, r)]
                work[g, r, ra, 256:384] = jnp.where(left, a, pltpu.roll(b, 64, 1))
                work[g, r, rb, 256:384] = jnp.where(left, pltpu.roll(a, 64, 1), b)

    def push(slot):
        return remote(vec.at[slot], recv.at[me], osem.at[slot], orsem.at[me], (band, slot))

    def inverse(blk, s):
        slot = ((chip + 1 - s // 2) % 2) * 2 + (core + s % 2 + s // 2) % 2
        q = jnp.concatenate([ytrans(work[slot, r]) for r in range(planes)], axis=0)
        w = ztrans(q).reshape(planes, ng, width) * buf[blk, slot]

        @pl.when(blk == 0)
        def _():
            acc[slot] = w

        @pl.when(blk == 1)
        def _():
            acc[slot] += w

        @pl.when(blk == 2)
        def _():
            hi, lo = split((acc[slot] + w).reshape(planes * ng, width))
            out = -(mm(hi, s_ref[...]) + mm(lo, s_ref[...]))
            vec[slot] = out.reshape(planes, ng, s_ref.shape[-1])

            @pl.when(s < 3)
            def _():
                push(slot).start()

    def block(blk, _):
        @pl.when(blk == 0)
        def _():
            local.wait()

        @pl.when(blk > 0)
        def _():
            relay(blk)

        @pl.when(blk == 1)
        def _():
            spread(2)

        def fwd(s, _):
            forward(blk, s)
            return 0

        def mid(t, _):
            xconv(t)
            return 0

        def inv(s, _):
            inverse(blk, s)
            return 0

        lax.fori_loop(0, 4, fwd, 0)
        lax.fori_loop(0, ng // 16, mid, 0)
        lax.fori_loop(0, 4, inv, 0)
        return 0

    lax.fori_loop(0, 3, block, 0)

    o_ref[me] = vec[me]
    for slot in (sib, cross, far):
        remote(vec.at[slot], recv.at[slot], osem.at[slot], orsem.at[slot], (band, slot)).wait()
        o_ref[slot] = recv[slot]
    for blk in range(3):
        for lane, target in ((0, sib), (1, cross), (2, sib)):
            share(blk, lane, me, own_ref, target).wait_send()
    remote(own_ref, buf.at[1, me], nsem.at[0], rsem.at[1, me], (above, me)).wait_send()
    remote(own_ref, buf.at[2, me], nsem.at[1], rsem.at[2, me], (below, me)).wait_send()


def lane_tables(ng, bands):
    w = bands * ng
    half, bz = [], []
    for lo, hi in ((0, 128), (128, w)):
        for h in range(2):
            half.append(np.full(hi - lo, h))
            bz.append(np.arange(lo, hi))
    half, bz = np.concatenate(half), np.concatenate(bz)
    return half, bz // ng, bz % ng


def solve(own, bands, groups):
    planes, ng, width = own.shape
    half, bnd, zed = lane_tables(ng, bands)
    ht = hartley(ng)
    th, tl = split_const(ht)
    same = (half[:, None] == half[None, :])
    zh, zl = split_const(np.where(same & (bnd[:, None] == bnd[None, :]), ht[zed[:, None], zed[None, :]], 0.0))
    ty = np.concatenate([th, th, tl], axis=1)
    copyz = same & (zed[:, None] == zed[None, :])
    sel = np.stack([copyz & (bnd[:, None] == g) for g in range(groups)]).astype(np.float32)
    s = np.zeros((width, 128), np.float32)
    s[np.arange(width), half * ng + zed] = 1.0
    kv = kernel_values(ng).astype(np.float32) / np.float32(ng**3)
    kb = np.tile(kv, (1, 1, bands))
    k1 = kb[:, :, :128]
    rest = kb[:, :, 128:].reshape(kb.shape[0], ng // 16, 2, 8, 64)
    k2 = np.concatenate([rest[:, :, 0], rest[:, :, 1]], axis=-1).reshape(kb.shape[0], ng // 2, 128)
    consts = [k1, k2, zh, zl, ty, sel.astype(jnp.bfloat16), s.astype(jnp.bfloat16)]
    full = (groups, planes, ng, width)
    f32, dma = jnp.float32, pltpu.SemaphoreType.DMA
    return pl.pallas_call(
        functools.partial(solve_kernel, ng),
        out_shape=jax.ShapeDtypeStruct((groups, planes, ng, 128), f32),
        in_specs=[pl.BlockSpec(memory_space=pltpu.VMEM)] * 8,
        out_specs=pl.BlockSpec(memory_space=pltpu.VMEM),
        scratch_shapes=[
            pltpu.VMEM((3,) + full, f32), pltpu.VMEM(full, f32), pltpu.VMEM(full, f32), pltpu.VMEM(full, f32),
            pltpu.VMEM((groups, planes, ng, 128), f32), pltpu.VMEM((groups, planes, ng, 128), f32),
            dma((3, groups)), dma((3, 3)), dma((2,)), dma((groups,)), dma((groups,)), dma(()),
        ],
        compiler_params=pltpu.CompilerParams(
            vmem_limit_bytes=56 * 1024 * 1024, collective_id=0, has_side_effects=True
        ),
        cost_estimate=pl.CostEstimate(flops=10**11, bytes_accessed=10**7, transcendentals=0),
        name="solve",
    )(own, *[jnp.asarray(c) for c in consts])


def on_device(orbitals):
    groups = lax.axis_size("grid")
    bands, local = orbitals.shape
    ncell = local * groups
    ng = round(ncell ** (1 / 3))
    xs = local // (ng * ng)
    planes = xs // 2
    t = orbitals.reshape(bands, 2, planes, ng, ng).transpose(2, 3, 1, 0, 4).reshape(planes, ng, 2, bands * ng)
    own = jnp.concatenate([t[:, :, 0, :128], t[:, :, 1, :128], t[:, :, 0, 128:], t[:, :, 1, 128:]], axis=-1)
    out = solve(own, bands, groups)
    vec = out[..., : 2 * ng].reshape(groups, planes, ng, 2, ng).transpose(0, 3, 1, 2, 4)
    vectors = vec.reshape(bands, local)
    terms = (
        lax.dot_general(
            lax.all_gather(orbitals, "band", axis=0, tiled=True),
            vectors,
            (((1,), (1,)), ((), ())),
            precision=lax.Precision.HIGHEST,
            preferred_element_type=jnp.float32,
        )
        / ncell
    )
    margin = lax.psum_scatter(terms, "grid", scatter_dimension=0, tiled=True)
    return (vectors, margin)


def solution(mesh):
    return jax.shard_map(
        on_device,
        mesh=mesh,
        in_specs=(P("band", "grid"),),
        out_specs=(P("band", "grid"), P("grid", "band")),
        check_vma=False,
    )
```
